32 devices in a mesh: seq: 8 (over y, x, core), batch: 4 (over z).
Axes of the slice: x: 2, y: 2, z: 4, core: 2. Of those that a mesh axis runs over, the one named last changes fastest.
Arguments:
- queries: bfloat16 [4096, 4096], P(('batch', 'seq')), parts along dimension 0, may hold values from -6 to 6
- key_vectors: bfloat16 [4096, 4096], P(('batch', 'seq')), parts along dimension 0, may hold values from -6 to 6
- value_vectors: bfloat16 [4096, 4096], P(('batch', 'seq')), parts along dimension 0, may hold values from -6 to 6
- residual_in: bfloat16 [4096, 4096], P(('batch', 'seq')), parts along dimension 0, may hold values from -6 to 6
- input_logit: float32 [8, 4096], P(None, ('batch', 'seq')), parts along dimension 1, may hold values from -8 to 300
- forget_logit: float32 [8, 4096], P(None, ('batch', 'seq')), parts along dimension 1, may hold values from -3 to 13
- mix_gain: float32 [4096], replicated, may hold values from 0.1 to 1.9
- ffn_gain: float32 [4096], replicated, may hold values from 0.1 to 1.9
- expert_gate: bfloat16 [8, 4096, 704], P('seq'), may hold values from -0.09375 to 0.09375
- expert_up: bfloat16 [8, 4096, 704], P('seq'), may hold values from -0.09375 to 0.09375
- expert_down: bfloat16 [8, 704, 4096], P('seq'), may hold values from -0.21875 to 0.21875
- routes: int32 [4096, 2], P(('batch', 'seq')), parts along dimension 0, may hold values from 0 to 7, all different within a row; in each aligned block of 128 rows (0 to 127, 128 to 255, ...) at most 64 rows name the same one
- route_weight: float32 [4096, 2], P(('batch', 'seq')), parts along dimension 0, may hold values from 0.2 to 1
Outputs:
- block_out: bfloat16 [4096, 4096], P(('batch', 'seq')), parts along dimension 0
The draws below stay inside these ranges and needn't reach their ends.
There are 4 independent parts, one for each index of `batch`. The reference program is written for one: setup_inputs(seed, part) draws one part's arguments, and reference() takes and returns one part's arrays. A program takes and returns all parts, laid end to end along the dimension named above; an argument that names none is the same for every part. Nothing has to cross between parts.
Inputs may be any that keep to these rules, and one draw needn't show every extreme that they name: `routes`: each row names two different experts. Within the rows of one device no expert is named by more than 64 rows, and in some device one expert is named by exactly 64 rows.
All inputs are finite; a program needn't handle non-finite values.
Results may differ from the reference program's by a relative error of at most 0.0081.
Values may be sent and summed in bfloat16 or wider, within the bound.
A program may use at most 128 MiB of HBM per device.

```python
import math
import jax
import jax.numpy as jnp
import numpy as np
from jax import lax

MIXER_HEADS = 8
DH = 512
D = 4096
FF = 704
TOK_DEV = 128
SEQUENCE_LENGTH = 1024
EXPERTS = 8
CAP = 64


def draw_forget_logit(key, part):
    random_child_keys = jax.random.split(jax.random.fold_in(key, 11), 6)
    chooser = jax.random.uniform(random_child_keys[0], (MIXER_HEADS, 1))
    quick_head = chooser < 0.5
    horizon = TOK_DEV * jax.random.uniform(random_child_keys[1], (MIXER_HEADS, 1), minval=0.15, maxval=0.25)
    slow_rate = jnp.log(1.0 / 0.7) / SEQUENCE_LENGTH * jnp.ones((MIXER_HEADS, 1), jnp.float32)
    base_rate = jnp.where(quick_head, 1.0 / horizon, slow_rate)
    blocks = SEQUENCE_LENGTH // TOK_DEV
    device_factor = jnp.exp(jax.random.uniform(random_child_keys[2], (MIXER_HEADS, blocks), minval=-0.7, maxval=0.7))
    device_factor = jnp.repeat(device_factor, TOK_DEV, axis=1)
    roughness = jax.random.uniform(random_child_keys[3], (MIXER_HEADS, SEQUENCE_LENGTH), minval=0.5, maxval=1.5)
    forget_decay_speed = base_rate * device_factor * roughness
    spike_locations = jax.random.randint(random_child_keys[4], (3,), 0, SEQUENCE_LENGTH)
    spike_present = jnp.any(jnp.arange(SEQUENCE_LENGTH)[None, :] == spike_locations[:, None], axis=0)[None, :]
    spike_frequency = jax.random.uniform(random_child_keys[5], (MIXER_HEADS, SEQUENCE_LENGTH), minval=0.22, maxval=0.69)
    forget_decay_speed = jnp.where(spike_present, spike_frequency, forget_decay_speed)
    return jnp.log(1.0 / jnp.expm1(forget_decay_speed)).astype(jnp.float32)


def draw_input_logit(key, part):
    random_child_keys = jax.random.split(jax.random.fold_in(key, 23), 5)
    drawn = jax.random.normal(random_child_keys[4], (MIXER_HEADS, SEQUENCE_LENGTH)) * 1.5 - 1.0
    return jnp.clip(drawn, -8.0, 8.0).astype(jnp.float32)


def block_levels(rng, dims, shards, least, largest):
    def one(dim, blocks):
        draws = jax.random.uniform(jax.random.fold_in(jax.random.fold_in(rng, 6), dim), (blocks,), jnp.float32, least / len(shards), largest / len(shards))
        return jnp.repeat(jnp.exp(draws), dims[dim] // blocks).reshape((-1,) + (1,) * (len(dims) - dim - 1))

    gain = one(*shards[0])
    for cut in shards[1:]:
        gain = gain * one(*cut)
    return gain


def shared_out(key, own, number, rows, number_of, top, reach, lean):
    sequence = jax.random.permutation(key, number_of)
    crowded, common = portions_of(number_of, rows * top, reach, lean, True), portions_of(number_of, rows * top, reach, lean, False)
    places = jnp.arange(number_of)

    def named(sizes, turn):
        used = int((sizes > 0).sum())
        fixed = max(1, used // 4)
        shifted = fixed + (places - fixed + turn * (used - fixed)) % max(1, number_of - fixed)
        return jnp.zeros((number_of,), jnp.int32).at[sequence[jnp.where(places < fixed, places, shifted)]].set(jnp.asarray(sizes, jnp.int32))

    sizes = jnp.where(number % 4 == 0, named(crowded, number // 4), named(common, number - number // 4 - 1))
    mixed = jax.random.permutation(jax.random.fold_in(own, 3), number_of)
    donor, receiver = mixed[0:number_of // 2 * 2:2], mixed[1:number_of // 2 * 2:2]
    slack = jnp.minimum(sizes[donor] - 1, reach - sizes[receiver]) // 2
    slack = jnp.where((donor == sequence[0]) | (receiver == sequence[0]) | (sizes[receiver] == 0), 0, jnp.maximum(slack, 0))
    shifted = jax.random.randint(jax.random.fold_in(own, 4), (number_of // 2,), 0, 1 << 20) % (slack + 1)
    sizes = sizes.at[donor].add(-shifted).at[receiver].add(shifted)
    members = jnp.searchsorted(jnp.cumsum(sizes), jnp.arange(rows * top), side="right").astype(jnp.int32)
    grid = members.reshape(top, rows).T
    grid = grid[jax.random.permutation(jax.random.fold_in(own, 1), rows)]
    turn = jax.random.randint(jax.random.fold_in(own, 2), (rows, 1), 0, top)
    return jnp.take_along_axis(grid, (jnp.arange(top)[None, :] + turn) % top, axis=1)


def portions_of(amount, total, limit, skew, full):
    weights = [(1 << 20) // math.isqrt(standing ** skew) + 1 for standing in range(1, amount + 1)]
    largest = limit if full else min(limit, max(-(-total // amount), total * weights[0] // sum(weights)))
    least = 1 if total - largest >= amount - 1 else 0
    given, surplus = [largest] + [least] * (amount - 1), total - largest - least * (amount - 1)
    while surplus > 0:
        free = [i for i in range(1, amount) if given[i] < largest] or [i for i in range(1, amount) if given[i] < limit]
        whole, remaining = sum([weights[i] for i in free]), surplus
        for i in free:
            more = min(limit - given[i], max(1, remaining * weights[i] // whole), surplus)
            given[i] = given[i] + more
            surplus = surplus - more
    return np.array(given)


def scatter_about(own_key, extent, spread, bound, cuts=(), kind=jnp.bfloat16):
    entries = spread * jax.random.normal(own_key, extent, jnp.float32)
    if cuts:
        entries = entries * block_levels(own_key, extent, cuts, -0.22, 0.18)
    return jnp.clip(entries, -bound, bound).astype(kind)


def setup_inputs(seed: int = 0, part: int = 0) -> dict:
    seeds = jax.random.split(jax.random.key(seed), 14)
    own_keys = jax.random.split(jax.random.fold_in(seeds[13], part), 14)
    queries = scatter_about(own_keys[0], (SEQUENCE_LENGTH, D), 1.0, 6.0, ((0, 8),))
    key_vectors = scatter_about(own_keys[1], (SEQUENCE_LENGTH, D), 1.0, 6.0, ((0, 8),))
    value_vectors = scatter_about(own_keys[2], (SEQUENCE_LENGTH, D), 1.0, 6.0, ((0, 8),))
    residual_in = scatter_about(own_keys[3], (SEQUENCE_LENGTH, D), 1.0, 6.0, ((0, 8),))
    input_logit = draw_input_logit(jax.random.fold_in(jax.random.fold_in(seeds[13], part), 71), part)
    forget_logit = draw_forget_logit(jax.random.fold_in(jax.random.fold_in(seeds[13], part), 71), part)
    mix_gain = jnp.clip(1.0 + 0.18 * jax.random.normal(seeds[6], (D,), jnp.float32), 0.1, 1.9)
    ffn_gain = jnp.clip(1.0 + 0.18 * jax.random.normal(seeds[7], (D,), jnp.float32), 0.1, 1.9)
    expert_gate = scatter_about(seeds[8], (EXPERTS, D, FF), D ** -0.5, 0.09375, ((0, 8),))
    expert_up = scatter_about(seeds[9], (EXPERTS, D, FF), D ** -0.5, 0.09375, ((0, 8),))
    expert_down = scatter_about(seeds[10], (EXPERTS, FF, D), FF ** -0.5, 0.21875, ((0, 8),))
    routes_keys = jax.random.split(jax.random.fold_in(own_keys[11], 1), SEQUENCE_LENGTH // TOK_DEV)
    routes_turns = jax.random.permutation(jax.random.fold_in(own_keys[11], 3), SEQUENCE_LENGTH // TOK_DEV)
    routes = jax.vmap(lambda own, number: shared_out(jax.random.fold_in(own_keys[11], 2), own, number, TOK_DEV, EXPERTS, 2, CAP, 2))(routes_keys, routes_turns).reshape((SEQUENCE_LENGTH, 2))
    route_weight = jnp.clip(0.2 + 0.8 * jax.random.uniform(own_keys[12], (SEQUENCE_LENGTH, 2), jnp.float32) ** block_levels(own_keys[12], (SEQUENCE_LENGTH, 2), ((0, 8),), -0.2, 0.2), 0.2, 1.0)
    return dict(queries=queries, key_vectors=key_vectors, value_vectors=value_vectors, residual_in=residual_in, input_logit=input_logit, forget_logit=forget_logit, mix_gain=mix_gain, ffn_gain=ffn_gain, expert_gate=expert_gate, expert_up=expert_up, expert_down=expert_down, routes=routes, route_weight=route_weight)


NEG_FILL = -1e+30
EPSILON = 1e-06

def join_states(earlier, later):
    total_early, state_early, normv_early, peak_early = earlier
    total_late, state_late, normv_late, peak_late = later
    carried = total_late + peak_early
    peak_new = jnp.maximum(carried, peak_late)
    scale_early = jnp.exp(carried - peak_new)
    scale_late = jnp.exp(peak_late - peak_new)
    state_new = scale_early[..., None] * state_early + scale_late[..., None] * state_late
    normv_new = scale_early * normv_early + scale_late * normv_late
    return (total_early + total_late, state_new, normv_new, peak_new)

def block_summary(keys_three, values_three, log_forget, input_gate):
    cumul_log = jnp.cumsum(log_forget, axis=1)
    tail_log = cumul_log[:, -1:] - cumul_log + input_gate
    peak_log = lax.optimization_barrier(jnp.max(tail_log, axis=1))
    weight = jnp.exp(tail_log - peak_log[:, None])
    weighted = keys_three.astype(jnp.float32) * jnp.transpose(weight)[:, :, None]
    rounded = lax.optimization_barrier(weighted.astype(jnp.bfloat16))
    state_mat = jnp.einsum('thd,the->hde', rounded.astype(jnp.float32), values_three.astype(jnp.float32))
    norm_vec = lax.optimization_barrier(jnp.sum(weighted, axis=0))
    total_log = jnp.broadcast_to(cumul_log[:, -1:], norm_vec.shape)
    peak_full = jnp.broadcast_to(peak_log[:, None], norm_vec.shape)
    return (total_log, state_mat, norm_vec, peak_full)

def block_output(queries_three, keys_three, values_three, log_forget, input_gate, carry_in):
    length_block = queries_three.shape[0]
    inverse_root = 1.0 / math.sqrt(queries_three.shape[2])
    cumul_log = jnp.cumsum(log_forget, axis=1)
    log_weight = cumul_log[:, :, None] - cumul_log[:, None, :] + input_gate[:, None, :]
    causal = jnp.arange(length_block)[:, None] >= jnp.arange(length_block)[None, :]
    log_weight = jnp.where(causal[None], log_weight, NEG_FILL)
    carry_total, carry_state, carry_norm, carry_peak = carry_in
    carried = cumul_log + carry_peak[:, 0:1]
    peak_log = jnp.maximum(lax.optimization_barrier(jnp.max(log_weight, axis=2)), carried)
    decay_mat = jnp.exp(log_weight - peak_log[:, :, None])
    query_float = queries_three.astype(jnp.float32)
    scores = jnp.einsum('thd,shd->hts', query_float, keys_three.astype(jnp.float32)) * inverse_root
    coef = decay_mat * scores
    denom_sum = lax.optimization_barrier(jnp.sum(coef, axis=2))
    coef_round = lax.optimization_barrier(coef.astype(jnp.bfloat16))
    numer_sum = jnp.einsum('hts,she->the', coef_round.astype(jnp.float32), values_three.astype(jnp.float32))
    carry_reach = jnp.exp(carried - peak_log) * inverse_root
    from_state = jnp.einsum('thd,hde->the', query_float, carry_state, precision=lax.Precision.HIGHEST)
    from_norm = jnp.einsum('thd,hd->ht', query_float, carry_norm, precision=lax.Precision.HIGHEST)
    numer_sum = numer_sum + jnp.transpose(carry_reach)[:, :, None] * from_state
    denom_sum = denom_sum + carry_reach * from_norm
    floor_sum = jnp.maximum(jnp.abs(denom_sum), 1.0)
    return numer_sum / jnp.transpose(floor_sum)[:, :, None]

def reference(queries, key_vectors, value_vectors, residual_in, input_logit, forget_logit, mix_gain, ffn_gain, expert_gate, expert_up, expert_down, routes, route_weight):
    log_forget = jax.nn.log_sigmoid(forget_logit)
    blocks = SEQUENCE_LENGTH // TOK_DEV

    def split_rows(array):
        return array.reshape(blocks, TOK_DEV, MIXER_HEADS, DH)

    def split_gates(array):
        return jnp.transpose(array.reshape(MIXER_HEADS, blocks, TOK_DEV), (1, 0, 2))
    initial = (jnp.zeros((MIXER_HEADS, DH), jnp.float32), jnp.zeros((MIXER_HEADS, DH, DH), jnp.float32), jnp.zeros((MIXER_HEADS, DH), jnp.float32), jnp.full((MIXER_HEADS, DH), NEG_FILL, jnp.float32))

    def advance(carry_in, pieces):
        query_block, key_block, value_block, forget_block, input_block = pieces
        result = block_output(query_block, key_block, value_block, forget_block, input_block, carry_in)
        carry_out = join_states(carry_in, block_summary(key_block, value_block, forget_block, input_block))
        return (carry_out, result)
    unused, mixer_out = lax.scan(advance, initial, (split_rows(queries), split_rows(key_vectors), split_rows(value_vectors), split_gates(log_forget), split_gates(input_logit)))
    mixer_out = mixer_out.reshape(SEQUENCE_LENGTH, D)
    mixer_square = lax.optimization_barrier(jnp.mean(mixer_out * mixer_out, axis=1, keepdims=True))
    updated = (residual_in.astype(jnp.float32) + mixer_out * lax.rsqrt(mixer_square + EPSILON) * mix_gain).astype(jnp.bfloat16)
    updated_float = updated.astype(jnp.float32)
    updated_square = lax.optimization_barrier(jnp.mean(updated_float * updated_float, axis=1, keepdims=True))
    normed = (updated_float * lax.rsqrt(updated_square + EPSILON) * ffn_gain).astype(jnp.bfloat16)
    flat_routes = routes.reshape(blocks, 2 * TOK_DEV)
    matches = (flat_routes[:, :, None] == jnp.arange(EXPERTS, dtype=jnp.int32)[None, None, :]).astype(jnp.int32)
    before = jnp.cumsum(matches, axis=1) - matches
    position = lax.optimization_barrier(jnp.sum(before * matches, axis=2))
    source_index = jnp.arange(blocks, dtype=jnp.int32)[:, None]
    slot_index = (flat_routes * (blocks * CAP) + source_index * CAP + position).reshape(SEQUENCE_LENGTH, 2).astype(jnp.int32)
    buffer_rows = jnp.zeros((EXPERTS * blocks * CAP, D), jnp.bfloat16)
    buffer_rows = buffer_rows.at[slot_index[:, 0]].set(normed).at[slot_index[:, 1]].set(normed)

    def run_expert(pieces):
        row_block, gate_weight, up_weight, down_weight = pieces
        gate_val = jnp.dot(row_block, gate_weight, preferred_element_type=jnp.float32)
        up_val = jnp.dot(row_block, up_weight, preferred_element_type=jnp.float32)
        hidden = (jax.nn.silu(gate_val) * up_val).astype(jnp.bfloat16)
        return jnp.dot(hidden, down_weight, preferred_element_type=jnp.float32).astype(jnp.bfloat16)
    outputs = lax.map(run_expert, (buffer_rows.reshape(EXPERTS, blocks * CAP, D), expert_gate, expert_up, expert_down)).reshape(EXPERTS * blocks * CAP, D)
    first_out = outputs[slot_index[:, 0]].astype(jnp.float32)
    second_out = outputs[slot_index[:, 1]].astype(jnp.float32)
    expert_mix = route_weight[:, 0:1] * first_out + route_weight[:, 1:2] * second_out
    return (updated_float + expert_mix).astype(jnp.bfloat16)
```

```python
import math

import jax
import jax.numpy as jnp
from jax import lax
from jax.sharding import PartitionSpec as P

EPSILON = 1e-06


def three_parts(array):
    high = lax.reduce_precision(array, 8, 7)
    rest = array - high
    middle = lax.reduce_precision(rest, 8, 7)
    low = rest - middle
    return [part.astype(jnp.bfloat16) for part in (high, middle, low)]


def head_mix(query, key, value, input_gate, forget_gate):
    positions, head_dim = query.shape
    cumul_log = jnp.cumsum(jax.nn.log_sigmoid(forget_gate))
    level = input_gate - cumul_log
    top = lax.cummax(level, axis=0)
    scores = lax.dot_general(
        query, key, (((1,), (1,)), ((), ())), preferred_element_type=jnp.float32
    )
    causal = jnp.arange(positions)[:, None] >= jnp.arange(positions)[None, :]
    decay = jnp.exp(jnp.minimum(level[None, :] - top[:, None], 0.0))
    coef = jnp.where(causal, decay * scores, 0.0) * (1.0 / math.sqrt(head_dim))
    denom_sum = jnp.sum(coef, axis=1, keepdims=True)
    numer_sum = jnp.dot(coef.astype(jnp.bfloat16), value, preferred_element_type=jnp.float32)
    return numer_sum / jnp.maximum(jnp.abs(denom_sum), 1.0)


def shards(
    queries,
    key_vectors,
    value_vectors,
    residual_in,
    input_logit,
    forget_logit,
    mix_gain,
    ffn_gain,
    expert_gate,
    expert_up,
    expert_down,
    routes,
    route_weight,
):
    tokens, model_width = queries.shape
    head_count = input_logit.shape[0]
    head_dim = model_width // head_count
    devices = lax.axis_size("seq")
    group = devices // head_count
    group_width = model_width // devices

    def by_head(array):
        moved = jnp.transpose(array.reshape(tokens, head_count, head_dim), (1, 0, 2))
        return jnp.repeat(moved, group, axis=0)

    gates = jnp.stack(three_parts(input_logit) + three_parts(forget_logit), axis=2)
    gates = jnp.pad(jnp.repeat(gates, group, axis=0), ((0, 0), (0, 0), (0, 122)))
    send = jnp.concatenate(
        (
            by_head(queries),
            by_head(key_vectors),
            jnp.transpose(value_vectors.reshape(tokens, devices, group_width), (1, 0, 2)),
            gates,
        ),
        axis=2,
    )
    got = lax.all_to_all(send, "seq", split_axis=0, concat_axis=0, tiled=True)
    got = got.reshape(devices * tokens, -1)
    gate_parts = got[:, 2 * head_dim + group_width :].astype(jnp.float32)
    mixed = head_mix(
        got[:, :head_dim],
        got[:, head_dim : 2 * head_dim],
        got[:, 2 * head_dim : 2 * head_dim + group_width],
        gate_parts[:, 0] + gate_parts[:, 1] + gate_parts[:, 2],
        gate_parts[:, 3] + gate_parts[:, 4] + gate_parts[:, 5],
    ).astype(jnp.bfloat16)
    mixer_out = lax.all_to_all(
        mixed.reshape(devices, tokens, group_width), "seq", split_axis=0, concat_axis=0, tiled=True
    )
    mixer_out = jnp.transpose(mixer_out, (1, 0, 2)).reshape(tokens, model_width)
    mixer_out = mixer_out.astype(jnp.float32)
    mixer_square = jnp.mean(mixer_out * mixer_out, axis=1, keepdims=True)
    updated = (
        residual_in.astype(jnp.float32) + mixer_out * lax.rsqrt(mixer_square + EPSILON) * mix_gain
    ).astype(jnp.bfloat16)
    updated_float = updated.astype(jnp.float32)
    updated_square = jnp.mean(updated_float * updated_float, axis=1, keepdims=True)
    normed = (updated_float * lax.rsqrt(updated_square + EPSILON) * ffn_gain).astype(jnp.bfloat16)
    capacity = 4 * tokens // devices
    flat_routes = routes.reshape(-1)
    matches = (flat_routes[:, None] == jnp.arange(devices, dtype=jnp.int32)[None, :]).astype(
        jnp.int32
    )
    before = jnp.cumsum(matches, axis=0) - matches
    position = jnp.sum(before * matches, axis=1)
    slot_index = (flat_routes * capacity + position).reshape(tokens, 2)
    columns = jnp.arange(devices * capacity, dtype=jnp.int32)
    pick_first = (slot_index[:, 0:1] == columns[None, :]).astype(jnp.bfloat16)
    pick_second = (slot_index[:, 1:2] == columns[None, :]).astype(jnp.bfloat16)
    spread = jnp.einsum(
        "tc,td->cd", pick_first + pick_second, normed, preferred_element_type=jnp.float32
    ).astype(jnp.bfloat16)
    outbound = spread.reshape(devices, capacity, model_width)
    block_in = lax.all_to_all(outbound, "seq", split_axis=0, concat_axis=0, tiled=True)
    row_block = block_in.reshape(-1, model_width)
    gate_val = jnp.dot(row_block, expert_gate[0], preferred_element_type=jnp.float32)
    up_val = jnp.dot(row_block, expert_up[0], preferred_element_type=jnp.float32)
    hidden = (jax.nn.silu(gate_val) * up_val).astype(jnp.bfloat16)
    result = jnp.dot(hidden, expert_down[0], preferred_element_type=jnp.float32).astype(
        jnp.bfloat16
    )
    inbound = lax.all_to_all(
        result.reshape(block_in.shape), "seq", split_axis=0, concat_axis=0, tiled=True
    )
    flat_back = inbound.reshape(devices * capacity, model_width)
    first_out = jnp.dot(pick_first, flat_back, preferred_element_type=jnp.float32)
    second_out = jnp.dot(pick_second, flat_back, preferred_element_type=jnp.float32)
    expert_mix = route_weight[:, 0:1] * first_out + route_weight[:, 1:2] * second_out
    return (updated_float + expert_mix).astype(jnp.bfloat16)


def solution(mesh):
    return jax.shard_map(
        shards,
        mesh=mesh,
        in_specs=(
            P(("batch", "seq"), None),
            P(("batch", "seq"), None),
            P(("batch", "seq"), None),
            P(("batch", "seq"), None),
            P(None, ("batch", "seq")),
            P(None, ("batch", "seq")),
            P(),
            P(),
            P("seq", None, None),
            P("seq", None, None),
            P("seq", None, None),
            P(("batch", "seq"), None),
            P(("batch", "seq"), None),
        ),
        out_specs=P(("batch", "seq"), None),
        check_vma=False,
    )
```

```python
import math

import jax
import jax.numpy as jnp
from jax import lax
from jax.experimental import pallas as pl
from jax.experimental.pallas import tpu as pltpu
from jax.sharding import PartitionSpec as P

EPSILON = 1e-06
PIECES = 4


def three_parts(array):
    high = lax.reduce_precision(array, 8, 7)
    rest = array - high
    middle = lax.reduce_precision(rest, 8, 7)
    low = rest - middle
    return [part.astype(jnp.bfloat16) for part in (high, middle, low)]


def head_mix(query, key, value, input_gate, forget_gate):
    positions, head_dim = query.shape
    cumul_log = jnp.cumsum(jax.nn.log_sigmoid(forget_gate))
    level = input_gate - cumul_log
    top = lax.cummax(level, axis=0)
    scores = lax.dot_general(
        query, key, (((1,), (1,)), ((), ())), preferred_element_type=jnp.float32
    )
    causal = jnp.arange(positions)[:, None] >= jnp.arange(positions)[None, :]
    decay = jnp.exp(jnp.minimum(level[None, :] - top[:, None], 0.0))
    coef = jnp.where(causal, decay * scores, 0.0) * (1.0 / math.sqrt(head_dim))
    denom_sum = jnp.sum(coef, axis=1, keepdims=True)
    numer_sum = jnp.dot(coef.astype(jnp.bfloat16), value, preferred_element_type=jnp.float32)
    return numer_sum / jnp.maximum(jnp.abs(denom_sum), 1.0)


def expert_kernel(
    normed,
    updated,
    pick,
    pick_back,
    slot_weight,
    gate_far,
    up_far,
    down_far,
    out,
    blocks,
    gate,
    up,
    down,
    rows,
    gate_sum,
    up_sum,
    hidden,
    core_out,
    own,
    core_in,
    hop_out,
    hop_in,
    keep,
    last_out,
    last_in,
    load_sem,
    gather_send,
    gather_recv,
    core_send,
    core_recv,
    hop_send,
    hop_recv,
    last_send,
    last_recv,
):
    me = lax.axis_index("seq")
    width = rows.shape[1]
    capacity = pick.shape[1]

    def peer(flip):
        total = 0
        for bit in (1, 2, 4):
            own_bit = lax.rem(lax.div(me, bit), 2)
            total = total + bit * ((1 - own_bit) if flip & bit else own_bit)
        return {"seq": total}

    def remote(source, target, send_sem, recv_sem, flip):
        return pltpu.make_async_remote_copy(
            src_ref=source,
            dst_ref=target,
            send_sem=send_sem,
            recv_sem=recv_sem,
            device_id=peer(flip),
            device_id_type=pl.DeviceIdType.MESH,
        )

    loads = [
        pltpu.make_async_copy(far, near, load_sem.at[i])
        for i, (far, near) in enumerate(((gate_far, gate), (up_far, up), (down_far, down)))
    ]
    for load in loads:
        load.start()
    barrier = pltpu.get_barrier_semaphore()
    for flip in (1, 2, 4):
        pl.semaphore_signal(
            barrier, inc=1, device_id=peer(flip), device_id_type=pl.DeviceIdType.MESH
        )
    pl.semaphore_wait(barrier, 3)

    def columns(piece):
        return pl.ds(piece * width, width)

    def block(slot, piece):
        return normed.at[:, columns(piece)] if slot == 0 else blocks.at[slot - 1, piece]

    gathers = {}
    for piece in range(PIECES):
        across = (4, 2) if piece % 2 == 0 else (2, 4)
        for slot, source, flip in (
            (1, 0, 1),
            (2, 0, 2),
            (4, 0, 4),
            (6,) + across,
            (3, 2, 1),
            (5, 4, 1),
            (7, 6, 1),
        ):
            gathers[slot, piece] = remote(
                block(source, piece),
                block(slot, piece),
                gather_send.at[slot - 1, piece],
                gather_recv.at[slot - 1, piece],
                flip,
            )

    def send_own(piece):
        for slot in (2, 4, 1):
            gathers[slot, piece].start()

    def first_products(piece):
        for slot in (1, 3, 5, 7):
            gathers[slot, piece].wait_recv()
        if piece == 0:
            loads[0].wait()
            loads[1].wait()
        for slot in range(8):
            rows[slot * capacity : (slot + 1) * capacity, :] = jnp.dot(
                pick[slot], block(slot, piece)[...], preferred_element_type=jnp.float32
            ).astype(jnp.bfloat16)
        for weight, total in ((gate, gate_sum), (up, up_sum)):
            term = jnp.dot(
                rows[...], weight[columns(piece), :], preferred_element_type=jnp.float32
            )
            total[...] = term if piece == 0 else total[...] + term

    send_own(0)
    send_own(1)
    for piece in range(PIECES):
        gathers[2, piece].wait_recv()
        gathers[4, piece].wait_recv()
        for slot in (6, 3, 5):
            gathers[slot, piece].start()
        if piece + 2 < PIECES:
            send_own(piece + 2)
        gathers[6, piece].wait_recv()
        gathers[7, piece].start()
        if piece > 0:
            first_products(piece - 1)
    first_products(PIECES - 1)
    gate_val = gate_sum[...]
    hidden[...] = (gate_val / (1.0 + jnp.exp(-gate_val)) * up_sum[...]).astype(jnp.bfloat16)
    loads[2].wait()

    core_copies, hop_copies, last_copies = {}, {}, {}

    def second_product(piece):
        rows[...] = (
            jnp.dot(hidden[...], down[:, columns(piece)], preferred_element_type=jnp.float32)
            * slot_weight[...]
        ).astype(jnp.bfloat16)
        for slot in (7, 5, 3, 1, 6, 4, 2, 0):
            part = jnp.dot(
                pick_back[slot],
                rows[slot * capacity : (slot + 1) * capacity, :],
                preferred_element_type=jnp.float32,
            ).astype(jnp.bfloat16)
            half = slot // 2
            if slot % 2 == 0:
                own[half, piece] = part
                continue
            core_out[half, piece] = part
            core_copies[half, piece] = remote(
                core_out.at[half, piece],
                core_in.at[half, piece],
                core_send.at[half, piece],
                core_recv.at[half, piece],
                1,
            )
            core_copies[half, piece].start()

    def first_hop(piece):
        first, second = (2, 4) if piece % 2 == 0 else (4, 2)
        for slot in (6, first, second, 0):
            half = slot // 2
            core_copies[half, piece].wait_recv()
            both = own[half, piece].astype(jnp.float32) + core_in[half, piece].astype(jnp.float32)
            if slot in (0, second):
                keep[0 if slot == 0 else 1, piece] = both
                continue
            place = 1 if slot == 6 else 0
            hop_out[place, piece] = both.astype(jnp.bfloat16)
            hop_copies[place, piece] = remote(
                hop_out.at[place, piece],
                hop_in.at[place, piece],
                hop_send.at[place, piece],
                hop_recv.at[place, piece],
                first,
            )
            hop_copies[place, piece].start()

    def second_hop(piece):
        second = 4 if piece % 2 == 0 else 2
        hop_copies[1, piece].wait_recv()
        last_out[piece] = (keep[1, piece] + hop_in[1, piece].astype(jnp.float32)).astype(
            jnp.bfloat16
        )
        last_copies[piece] = remote(
            last_out.at[piece], last_in.at[piece], last_send.at[piece], last_recv.at[piece], second
        )
        last_copies[piece].start()

    def finish(piece):
        hop_copies[0, piece].wait_recv()
        last_copies[piece].wait_recv()
        out[:, columns(piece)] = (
            updated[:, columns(piece)].astype(jnp.float32)
            + (
                keep[0, piece]
                + hop_in[0, piece].astype(jnp.float32)
                + last_in[piece].astype(jnp.float32)
            )
        ).astype(jnp.bfloat16)

    for piece in range(PIECES):
        second_product(piece)
        if piece > 0:
            first_hop(piece - 1)
    first_hop(PIECES - 1)
    for piece in range(PIECES):
        second_hop(piece)
        if piece > 0:
            finish(piece - 1)
    finish(PIECES - 1)
    for copies in (gathers, core_copies, hop_copies, last_copies):
        for copy in copies.values():
            copy.wait_send()


def cube_experts(normed, updated, pick, slot_weight, gate_weight, up_weight, down_weight):
    tokens, model_width = normed.shape
    hidden_width = gate_weight.shape[1]
    slots = slot_weight.shape[0]
    width = model_width // PIECES
    near = pl.BlockSpec(memory_space=pltpu.VMEM)
    far = pl.BlockSpec(memory_space=pl.ANY)

    def pieces(*lead, kind=jnp.bfloat16):
        return pltpu.VMEM(lead + (PIECES, tokens, width), kind)

    def flags(*shape):
        return pltpu.SemaphoreType.DMA(shape)

    return pl.pallas_call(
        expert_kernel,
        out_shape=jax.ShapeDtypeStruct((tokens, model_width), jnp.bfloat16),
        in_specs=[near] * 5 + [far] * 3,
        out_specs=near,
        scratch_shapes=[
            pieces(7),
            pltpu.VMEM(gate_weight.shape, jnp.bfloat16),
            pltpu.VMEM(up_weight.shape, jnp.bfloat16),
            pltpu.VMEM(down_weight.shape, jnp.bfloat16),
            pltpu.VMEM((slots, width), jnp.bfloat16),
            pltpu.VMEM((slots, hidden_width), jnp.float32),
            pltpu.VMEM((slots, hidden_width), jnp.float32),
            pltpu.VMEM((slots, hidden_width), jnp.bfloat16),
            pieces(4),
            pieces(4),
            pieces(4),
            pieces(2),
            pieces(2),
            pieces(2, kind=jnp.float32),
            pieces(),
            pieces(),
            flags(3),
            flags(7, PIECES),
            flags(7, PIECES),
            flags(4, PIECES),
            flags(4, PIECES),
            flags(2, PIECES),
            flags(2, PIECES),
            flags(PIECES),
            flags(PIECES),
        ],
        compiler_params=pltpu.CompilerParams(
            collective_id=1, has_side_effects=True, vmem_limit_bytes=67043328
        ),
    )(
        normed,
        updated,
        pick,
        jnp.transpose(pick, (0, 2, 1)),
        slot_weight,
        gate_weight,
        up_weight,
        down_weight,
    )


def shards(
    queries,
    key_vectors,
    value_vectors,
    residual_in,
    input_logit,
    forget_logit,
    mix_gain,
    ffn_gain,
    expert_gate,
    expert_up,
    expert_down,
    routes,
    route_weight,
):
    tokens, model_width = queries.shape
    head_count = input_logit.shape[0]
    head_dim = model_width // head_count
    devices = lax.axis_size("seq")
    group = devices // head_count
    group_width = model_width // devices

    def by_head(array):
        moved = jnp.transpose(array.reshape(tokens, head_count, head_dim), (1, 0, 2))
        return jnp.repeat(moved, group, axis=0)

    capacity = 4 * tokens // devices
    flat_routes = routes.reshape(-1)
    matches = (flat_routes[:, None] == jnp.arange(devices, dtype=jnp.int32)[None, :]).astype(
        jnp.int32
    )
    before = jnp.cumsum(matches, axis=0) - matches
    position = jnp.sum(before * matches, axis=1)
    position = position.reshape(tokens, 2)
    slot_index = (flat_routes * capacity + position.reshape(-1)).reshape(tokens, 2)
    gates = jnp.stack(three_parts(input_logit) + three_parts(forget_logit), axis=2)
    gates = jnp.repeat(gates, group, axis=0)
    notes = jnp.concatenate(
        [routes.astype(jnp.bfloat16), position.astype(jnp.bfloat16)] + three_parts(route_weight),
        axis=1,
    )
    notes = jnp.broadcast_to(notes[None], (devices,) + notes.shape)
    gates = jnp.concatenate((gates, notes), axis=2)
    gates = jnp.pad(gates, ((0, 0), (0, 0), (0, 128 - gates.shape[2])))
    send = jnp.concatenate(
        (
            by_head(queries),
            by_head(key_vectors),
            jnp.transpose(value_vectors.reshape(tokens, devices, group_width), (1, 0, 2)),
            gates,
        ),
        axis=2,
    )
    got = lax.all_to_all(send, "seq", split_axis=0, concat_axis=0, tiled=True)
    got = got.reshape(devices * tokens, -1)
    gate_parts = got[:, 2 * head_dim + group_width :].astype(jnp.float32)
    mixed = head_mix(
        got[:, :head_dim],
        got[:, head_dim : 2 * head_dim],
        got[:, 2 * head_dim : 2 * head_dim + group_width],
        gate_parts[:, 0] + gate_parts[:, 1] + gate_parts[:, 2],
        gate_parts[:, 3] + gate_parts[:, 4] + gate_parts[:, 5],
    ).astype(jnp.bfloat16)
    mixer_out = lax.all_to_all(
        mixed.reshape(devices, tokens, group_width), "seq", split_axis=0, concat_axis=0, tiled=True
    )
    mixer_out = jnp.transpose(mixer_out, (1, 0, 2)).reshape(tokens, model_width)
    mixer_out = mixer_out.astype(jnp.float32)
    mixer_square = jnp.mean(mixer_out * mixer_out, axis=1, keepdims=True)
    updated = (
        residual_in.astype(jnp.float32) + mixer_out * lax.rsqrt(mixer_square + EPSILON) * mix_gain
    ).astype(jnp.bfloat16)
    updated_float = updated.astype(jnp.float32)
    updated_square = jnp.mean(updated_float * updated_float, axis=1, keepdims=True)
    normed = (updated_float * lax.rsqrt(updated_square + EPSILON) * ffn_gain).astype(jnp.bfloat16)
    if devices == 8:
        me = lax.axis_index("seq")
        told = gate_parts[:, 6:16].reshape(devices, tokens, 10)
        told = told[jnp.bitwise_xor(me, jnp.arange(devices, dtype=jnp.int32))]
        mine = me.astype(jnp.float32)
        places = jnp.where(told[:, :, 0:2] == mine, told[:, :, 2:4], -1.0)
        slots = jnp.arange(capacity, dtype=jnp.float32)[None, :, None]
        pick_one = places[:, None, :, 0] == slots
        pick_two = places[:, None, :, 1] == slots
        weights = told[:, :, 4:6] + told[:, :, 6:8] + told[:, :, 8:10]
        slot_weight = jnp.sum(
            jnp.where(pick_one, weights[:, None, :, 0], 0.0)
            + jnp.where(pick_two, weights[:, None, :, 1], 0.0),
            axis=2,
        ).reshape(devices * capacity, 1)
        pick = jnp.logical_or(pick_one, pick_two).astype(jnp.bfloat16)
        return cube_experts(
            normed, updated, pick, slot_weight, expert_gate[0], expert_up[0], expert_down[0]
        )
    columns = jnp.arange(devices * capacity, dtype=jnp.int32)
    pick_first = (slot_index[:, 0:1] == columns[None, :]).astype(jnp.bfloat16)
    pick_second = (slot_index[:, 1:2] == columns[None, :]).astype(jnp.bfloat16)
    spread = jnp.einsum(
        "tc,td->cd", pick_first + pick_second, normed, preferred_element_type=jnp.float32
    ).astype(jnp.bfloat16)
    outbound = spread.reshape(devices, capacity, model_width)
    block_in = lax.all_to_all(outbound, "seq", split_axis=0, concat_axis=0, tiled=True)
    row_block = block_in.reshape(-1, model_width)
    gate_val = jnp.dot(row_block, expert_gate[0], preferred_element_type=jnp.float32)
    up_val = jnp.dot(row_block, expert_up[0], preferred_element_type=jnp.float32)
    hidden = (jax.nn.silu(gate_val) * up_val).astype(jnp.bfloat16)
    result = jnp.dot(hidden, expert_down[0], preferred_element_type=jnp.float32).astype(
        jnp.bfloat16
    )
    inbound = lax.all_to_all(
        result.reshape(block_in.shape), "seq", split_axis=0, concat_axis=0, tiled=True
    )
    flat_back = inbound.reshape(devices * capacity, model_width)
    first_out = jnp.dot(pick_first, flat_back, preferred_element_type=jnp.float32)
    second_out = jnp.dot(pick_second, flat_back, preferred_element_type=jnp.float32)
    expert_mix = route_weight[:, 0:1] * first_out + route_weight[:, 1:2] * second_out
    return (updated_float + expert_mix).astype(jnp.bfloat16)


def solution(mesh):
    return jax.shard_map(
        shards,
        mesh=mesh,
        in_specs=(
            P(("batch", "seq"), None),
            P(("batch", "seq"), None),
            P(("batch", "seq"), None),
            P(("batch", "seq"), None),
            P(None, ("batch", "seq")),
            P(None, ("batch", "seq")),
            P(),
            P(),
            P("seq", None, None),
            P("seq", None, None),
            P("seq", None, None),
            P(("batch", "seq"), None),
            P(("batch", "seq"), None),
        ),
        out_specs=P(("batch", "seq"), None),
        check_vma=False,
    )
```

```python
import functools
import math

import jax
import jax.numpy as jnp
from jax import lax
from jax.experimental import pallas as pl
from jax.experimental.pallas import tpu as pltpu
from jax.sharding import PartitionSpec as P

EPSILON = 1e-06
PIECES = 4


def exchange_kernel(moves, devices, *refs):
    count = len(moves)
    sources, targets = refs[:count], refs[count : 2 * count]
    send_sem, recv_sem, local_sem = refs[2 * count :]
    me = lax.axis_index("seq")
    others = [lax.rem(me + step, devices) for step in range(1, devices)]
    barrier = pltpu.get_barrier_semaphore()
    for other in others:
        pl.semaphore_signal(
            barrier, inc=1, device_id={"seq": other}, device_id_type=pl.DeviceIdType.MESH
        )
    pl.semaphore_wait(barrier, devices - 1)
    copies = []
    for i, (take, put) in enumerate(moves):
        for step, other in enumerate(others):
            copies.append(
                pltpu.make_async_remote_copy(
                    src_ref=take(sources[i], other),
                    dst_ref=put(targets[i], me),
                    send_sem=send_sem.at[i, step],
                    recv_sem=recv_sem.at[i, step],
                    device_id={"seq": other},
                    device_id_type=pl.DeviceIdType.MESH,
                )
            )
            copies[-1].start()
    for i, (take, put) in enumerate(moves):
        copies.append(
            pltpu.make_async_copy(take(sources[i], me), put(targets[i], me), local_sem.at[i])
        )
        copies[-1].start()
    for copy in copies:
        copy.wait()


def exchange(moves, devices, number, sources, shapes):
    far = pl.BlockSpec(memory_space=pl.ANY)
    count = len(moves)
    return pl.pallas_call(
        functools.partial(exchange_kernel, moves, devices),
        out_shape=shapes,
        in_specs=[far] * count,
        out_specs=[far] * count,
        scratch_shapes=[
            pltpu.SemaphoreType.DMA((count, devices - 1)),
            pltpu.SemaphoreType.DMA((count, devices - 1)),
            pltpu.SemaphoreType.DMA((count,)),
        ],
        compiler_params=pltpu.CompilerParams(collective_id=number, has_side_effects=True),
    )(*sources)


def head_mix(query, key, value, input_gate, forget_gate):
    positions, head_dim = query.shape
    cumul_log = jnp.cumsum(jax.nn.log_sigmoid(forget_gate))
    level = input_gate - cumul_log
    top = lax.cummax(level, axis=0)
    scores = lax.dot_general(
        query, key, (((1,), (1,)), ((), ())), preferred_element_type=jnp.float32
    )
    causal = jnp.arange(positions)[:, None] >= jnp.arange(positions)[None, :]
    decay = jnp.exp(jnp.minimum(level[None, :] - top[:, None], 0.0))
    coef = jnp.where(causal, decay * scores, 0.0) * (1.0 / math.sqrt(head_dim))
    denom_sum = jnp.sum(coef, axis=1, keepdims=True)
    numer_sum = jnp.dot(coef.astype(jnp.bfloat16), value, preferred_element_type=jnp.float32)
    return numer_sum / jnp.maximum(jnp.abs(denom_sum), 1.0)


def expert_kernel(
    normed,
    updated,
    pick,
    pick_back,
    slot_weight,
    gate_far,
    up_far,
    down_far,
    out,
    blocks,
    gate,
    up,
    down,
    rows,
    gate_sum,
    up_sum,
    hidden,
    core_out,
    own,
    core_in,
    hop_out,
    hop_in,
    keep,
    last_out,
    last_in,
    load_sem,
    gather_send,
    gather_recv,
    core_send,
    core_recv,
    hop_send,
    hop_recv,
    last_send,
    last_recv,
):
    me = lax.axis_index("seq")
    width = rows.shape[1]
    capacity = pick.shape[1]

    def peer(flip):
        total = 0
        for bit in (1, 2, 4):
            own_bit = lax.rem(lax.div(me, bit), 2)
            total = total + bit * ((1 - own_bit) if flip & bit else own_bit)
        return {"seq": total}

    def remote(source, target, send_sem, recv_sem, flip):
        return pltpu.make_async_remote_copy(
            src_ref=source,
            dst_ref=target,
            send_sem=send_sem,
            recv_sem=recv_sem,
            device_id=peer(flip),
            device_id_type=pl.DeviceIdType.MESH,
        )

    loads = [
        pltpu.make_async_copy(far, near, load_sem.at[i])
        for i, (far, near) in enumerate(((gate_far, gate), (up_far, up), (down_far, down)))
    ]
    for load in loads:
        load.start()
    barrier = pltpu.get_barrier_semaphore()
    for flip in (1, 2, 4):
        pl.semaphore_signal(
            barrier, inc=1, device_id=peer(flip), device_id_type=pl.DeviceIdType.MESH
        )
    pl.semaphore_wait(barrier, 3)

    def columns(piece):
        return pl.ds(piece * width, width)

    def block(slot, piece):
        return normed.at[:, columns(piece)] if slot == 0 else blocks.at[slot - 1, piece]

    gathers = {}
    for piece in range(PIECES):
        across = (4, 2) if piece % 2 == 0 else (2, 4)
        for slot, source, flip in (
            (1, 0, 1),
            (2, 0, 2),
            (4, 0, 4),
            (6,) + across,
            (3, 2, 1),
            (5, 4, 1),
            (7, 6, 1),
        ):
            gathers[slot, piece] = remote(
                block(source, piece),
                block(slot, piece),
                gather_send.at[slot - 1, piece],
                gather_recv.at[slot - 1, piece],
                flip,
            )

    def send_own(piece):
        for slot in (2, 4, 1):
            gathers[slot, piece].start()

    def first_products(piece):
        for slot in (1, 3, 5, 7):
            gathers[slot, piece].wait_recv()
        if piece == 0:
            loads[0].wait()
            loads[1].wait()
        for slot in range(8):
            rows[slot * capacity : (slot + 1) * capacity, :] = jnp.dot(
                pick[slot], block(slot, piece)[...], preferred_element_type=jnp.float32
            ).astype(jnp.bfloat16)
        for weight, total in ((gate, gate_sum), (up, up_sum)):
            term = lax.dot_general(
                rows[...],
                weight[:, columns(piece)],
                (((1,), (1,)), ((), ())),
                preferred_element_type=jnp.float32,
            )
            total[...] = term if piece == 0 else total[...] + term

    send_own(0)
    send_own(1)
    for piece in range(PIECES):
        gathers[2, piece].wait_recv()
        gathers[4, piece].wait_recv()
        for slot in (6, 3, 5):
            gathers[slot, piece].start()
        if piece + 2 < PIECES:
            send_own(piece + 2)
        gathers[6, piece].wait_recv()
        gathers[7, piece].start()
        if piece > 0:
            first_products(piece - 1)
    first_products(PIECES - 1)
    gate_val = gate_sum[...]
    hidden[...] = (gate_val / (1.0 + jnp.exp(-gate_val)) * up_sum[...]).astype(jnp.bfloat16)
    loads[2].wait()

    core_copies, hop_copies, last_copies = {}, {}, {}

    def second_product(piece):
        rows[...] = (
            jnp.dot(hidden[...], down[:, columns(piece)], preferred_element_type=jnp.float32)
            * slot_weight[...]
        ).astype(jnp.bfloat16)
        for slot in (7, 5, 3, 1, 6, 4, 2, 0):
            part = jnp.dot(
                pick_back[slot],
                rows[slot * capacity : (slot + 1) * capacity, :],
                preferred_element_type=jnp.float32,
            ).astype(jnp.bfloat16)
            half = slot // 2
            if slot % 2 == 0:
                own[half, piece] = part
                continue
            core_out[half, piece] = part
            core_copies[half, piece] = remote(
                core_out.at[half, piece],
                core_in.at[half, piece],
                core_send.at[half, piece],
                core_recv.at[half, piece],
                1,
            )
            core_copies[half, piece].start()

    def first_hop(piece):
        first, second = (2, 4) if piece % 2 == 0 else (4, 2)
        for slot in (6, first, second, 0):
            half = slot // 2
            core_copies[half, piece].wait_recv()
            both = own[half, piece].astype(jnp.float32) + core_in[half, piece].astype(jnp.float32)
            if slot in (0, second):
                keep[0 if slot == 0 else 1, piece] = both
                continue
            place = 1 if slot == 6 else 0
            hop_out[place, piece] = both.astype(jnp.bfloat16)
            hop_copies[place, piece] = remote(
                hop_out.at[place, piece],
                hop_in.at[place, piece],
                hop_send.at[place, piece],
                hop_recv.at[place, piece],
                first,
            )
            hop_copies[place, piece].start()

    def second_hop(piece):
        second = 4 if piece % 2 == 0 else 2
        hop_copies[1, piece].wait_recv()
        last_out[piece] = (keep[1, piece] + hop_in[1, piece].astype(jnp.float32)).astype(
            jnp.bfloat16
        )
        last_copies[piece] = remote(
            last_out.at[piece], last_in.at[piece], last_send.at[piece], last_recv.at[piece], second
        )
        last_copies[piece].start()

    def finish(piece):
        hop_copies[0, piece].wait_recv()
        last_copies[piece].wait_recv()
        out[:, columns(piece)] = (
            updated[:, columns(piece)].astype(jnp.float32)
            + (
                keep[0, piece]
                + hop_in[0, piece].astype(jnp.float32)
                + last_in[piece].astype(jnp.float32)
            )
        ).astype(jnp.bfloat16)

    for piece in range(PIECES):
        second_product(piece)
        if piece > 0:
            first_hop(piece - 1)
    first_hop(PIECES - 1)
    for piece in range(PIECES):
        second_hop(piece)
        if piece > 0:
            finish(piece - 1)
    finish(PIECES - 1)
    for copies in (gathers, core_copies, hop_copies, last_copies):
        for copy in copies.values():
            copy.wait_send()


def cube_experts(normed, updated, pick, slot_weight, gate_weight, up_weight, down_weight):
    tokens, model_width = normed.shape
    hidden_width = gate_weight.shape[0]
    slots = slot_weight.shape[0]
    width = model_width // PIECES
    near = pl.BlockSpec(memory_space=pltpu.VMEM)
    far = pl.BlockSpec(memory_space=pl.ANY)

    def pieces(*lead, kind=jnp.bfloat16):
        return pltpu.VMEM(lead + (PIECES, tokens, width), kind)

    def flags(*shape):
        return pltpu.SemaphoreType.DMA(shape)

    return pl.pallas_call(
        expert_kernel,
        out_shape=jax.ShapeDtypeStruct((tokens, model_width), jnp.bfloat16),
        in_specs=[near] * 5 + [far] * 3,
        out_specs=near,
        scratch_shapes=[
            pieces(7),
            pltpu.VMEM(gate_weight.shape, jnp.bfloat16),
            pltpu.VMEM(up_weight.shape, jnp.bfloat16),
            pltpu.VMEM(down_weight.shape, jnp.bfloat16),
            pltpu.VMEM((slots, width), jnp.bfloat16),
            pltpu.VMEM((slots, hidden_width), jnp.float32),
            pltpu.VMEM((slots, hidden_width), jnp.float32),
            pltpu.VMEM((slots, hidden_width), jnp.bfloat16),
            pieces(4),
            pieces(4),
            pieces(4),
            pieces(2),
            pieces(2),
            pieces(2, kind=jnp.float32),
            pieces(),
            pieces(),
            flags(3),
            flags(7, PIECES),
            flags(7, PIECES),
            flags(4, PIECES),
            flags(4, PIECES),
            flags(2, PIECES),
            flags(2, PIECES),
            flags(PIECES),
            flags(PIECES),
        ],
        compiler_params=pltpu.CompilerParams(
            collective_id=1, has_side_effects=True, vmem_limit_bytes=67043328
        ),
    )(
        normed,
        updated,
        pick,
        jnp.transpose(pick, (0, 2, 1)),
        slot_weight,
        gate_weight,
        up_weight,
        down_weight,
    )


def shards(
    queries,
    key_vectors,
    value_vectors,
    residual_in,
    input_logit,
    forget_logit,
    mix_gain,
    ffn_gain,
    expert_gate,
    expert_up,
    expert_down,
    routes,
    route_weight,
):
    tokens, model_width = queries.shape
    head_count = input_logit.shape[0]
    head_dim = model_width // head_count
    devices = lax.axis_size("seq")
    group = devices // head_count
    group_width = model_width // devices

    capacity = 4 * tokens // devices
    flat_routes = routes.reshape(-1)
    matches = (flat_routes[:, None] == jnp.arange(devices, dtype=jnp.int32)[None, :]).astype(
        jnp.int32
    )
    before = jnp.cumsum(matches, axis=0) - matches
    position = jnp.sum(before * matches, axis=1)
    position = position.reshape(tokens, 2)
    slot_index = (flat_routes * capacity + position.reshape(-1)).reshape(tokens, 2)
    notes = jnp.stack(
        (jnp.repeat(input_logit, group, axis=0), jnp.repeat(forget_logit, group, axis=0)), axis=1
    )
    routing = jnp.concatenate(
        (routes.astype(jnp.float32), position.astype(jnp.float32), route_weight), axis=1
    )
    routing = jnp.broadcast_to(jnp.transpose(routing)[None], (devices, 6, tokens))
    notes = jnp.concatenate((notes, routing), axis=1)

    def columns_of(width, share):
        return lambda ref, other: ref.at[
            :, pl.ds(pl.multiple_of((other // share) * width, width), width)
        ]

    def rows_from(ref, origin):
        return ref.at[pl.ds(pl.multiple_of(origin * tokens, tokens), tokens), :]

    def entry(ref, other):
        return ref.at[other]

    head_columns = columns_of(head_dim, group)
    own_columns = columns_of(group_width, 1)
    tall = devices * tokens
    told, key_all, query_all, value_all = exchange(
        (
            (entry, entry),
            (head_columns, rows_from),
            (head_columns, rows_from),
            (own_columns, rows_from),
        ),
        devices,
        2,
        (notes, key_vectors, queries, value_vectors),
        (
            jax.ShapeDtypeStruct(notes.shape, jnp.float32),
            jax.ShapeDtypeStruct((tall, head_dim), jnp.bfloat16),
            jax.ShapeDtypeStruct((tall, head_dim), jnp.bfloat16),
            jax.ShapeDtypeStruct((tall, group_width), jnp.bfloat16),
        ),
    )
    mixed = head_mix(
        query_all, key_all, value_all, told[:, 0].reshape(-1), told[:, 1].reshape(-1)
    ).astype(jnp.bfloat16)
    (mixer_out,) = exchange(
        ((rows_from, own_columns),),
        devices,
        3,
        (mixed,),
        (jax.ShapeDtypeStruct((tokens, model_width), jnp.bfloat16),),
    )
    mixer_out = mixer_out.astype(jnp.float32)
    mixer_square = jnp.mean(mixer_out * mixer_out, axis=1, keepdims=True)
    updated = (
        residual_in.astype(jnp.float32) + mixer_out * lax.rsqrt(mixer_square + EPSILON) * mix_gain
    ).astype(jnp.bfloat16)
    updated_float = updated.astype(jnp.float32)
    updated_square = jnp.mean(updated_float * updated_float, axis=1, keepdims=True)
    normed = (updated_float * lax.rsqrt(updated_square + EPSILON) * ffn_gain).astype(jnp.bfloat16)
    if devices == 8:
        me = lax.axis_index("seq")
        told = told[jnp.bitwise_xor(me, jnp.arange(devices, dtype=jnp.int32))]
        mine = me.astype(jnp.float32)
        places = jnp.where(told[:, 2:4] == mine, told[:, 4:6], -1.0)
        slots = jnp.arange(capacity, dtype=jnp.float32)[None, :, None]
        pick_one = places[:, 0:1] == slots
        pick_two = places[:, 1:2] == slots
        slot_weight = jnp.sum(
            jnp.where(pick_one, told[:, 6:7], 0.0) + jnp.where(pick_two, told[:, 7:8], 0.0),
            axis=2,
        ).reshape(devices * capacity, 1)
        pick = jnp.logical_or(pick_one, pick_two).astype(jnp.bfloat16)
        return cube_experts(
            normed,
            updated,
            pick,
            slot_weight,
            jnp.transpose(expert_gate[0]),
            jnp.transpose(expert_up[0]),
            expert_down[0],
        )
    columns = jnp.arange(devices * capacity, dtype=jnp.int32)
    pick_first = (slot_index[:, 0:1] == columns[None, :]).astype(jnp.bfloat16)
    pick_second = (slot_index[:, 1:2] == columns[None, :]).astype(jnp.bfloat16)
    spread = jnp.einsum(
        "tc,td->cd", pick_first + pick_second, normed, preferred_element_type=jnp.float32
    ).astype(jnp.bfloat16)
    outbound = spread.reshape(devices, capacity, model_width)
    block_in = lax.all_to_all(outbound, "seq", split_axis=0, concat_axis=0, tiled=True)
    row_block = block_in.reshape(-1, model_width)
    gate_val = jnp.dot(row_block, expert_gate[0], preferred_element_type=jnp.float32)
    up_val = jnp.dot(row_block, expert_up[0], preferred_element_type=jnp.float32)
    hidden = (jax.nn.silu(gate_val) * up_val).astype(jnp.bfloat16)
    result = jnp.dot(hidden, expert_down[0], preferred_element_type=jnp.float32).astype(
        jnp.bfloat16
    )
    inbound = lax.all_to_all(
        result.reshape(block_in.shape), "seq", split_axis=0, concat_axis=0, tiled=True
    )
    flat_back = inbound.reshape(devices * capacity, model_width)
    first_out = jnp.dot(pick_first, flat_back, preferred_element_type=jnp.float32)
    second_out = jnp.dot(pick_second, flat_back, preferred_element_type=jnp.float32)
    expert_mix = route_weight[:, 0:1] * first_out + route_weight[:, 1:2] * second_out
    return (updated_float + expert_mix).astype(jnp.bfloat16)


def solution(mesh):
    return jax.shard_map(
        shards,
        mesh=mesh,
        in_specs=(
            P(("batch", "seq"), None),
            P(("batch", "seq"), None),
            P(("batch", "seq"), None),
            P(("batch", "seq"), None),
            P(None, ("batch", "seq")),
            P(None, ("batch", "seq")),
            P(),
            P(),
            P("seq", None, None),
            P("seq", None, None),
            P("seq", None, None),
            P(("batch", "seq"), None),
            P(("batch", "seq"), None),
        ),
        out_specs=P(("batch", "seq"), None),
        check_vma=False,
    )
```
